128 devices in a mesh: dp: 16 (over y_hi, x, core), mp: 8 (over z, y_lo).
Axes of the slice: x: 4, y: 4 (y_hi: 2, y_lo: 2; y = y_hi * 2 + y_lo), z: 4, core: 2. Of those that a mesh axis runs over, the one named last changes fastest.
Arguments:
- hidden_states: bfloat16 [65536, 4096], P('dp', 'mp'), may hold values from -1 to 1
- factor_values: bfloat16 [65536, 128], P('dp', 'mp'), may hold values from 0.029907227 to 0.13964844
- class_ids: int32 [65536, 128], P('dp', 'mp'), may hold values from 0 to 128255, as said below
- centers: int32 [3], replicated, may hold values from 0 to 65535
Outputs:
- min_distance: float32 [65536], P(('dp', 'mp'))
- weight_means: float32 [3], replicated
The draws below stay inside these ranges and needn't reach their ends.
Inputs may be any that keep to these rules, and one draw needn't show every extreme that they name: `centers`: each value is a sample index. `class_ids`: entries k * 16 to (k + 1) * 16 - 1 of a row hold distinct classes of the k-th of 8 equal ranges of the vocabulary.
All inputs are finite; a program needn't handle non-finite values.
Results may differ from the reference program's by a relative error of at most 0.00095.
Values may be sent and summed in bfloat16 or wider, within the bound.
A program may use at most 64 MiB of HBM per device.

```python
import jax
import jax.numpy as jnp
from jax import lax

D = 4096
VOCAB = 128256
K_LOC = 16
STEPS = 3
SAMP_DEV = 512
TOPK = 128
POOL = 65536


def draw_hidden_states(key, part):
    key_shared, key_noise = jax.random.split(key, 2)
    shared = jax.random.normal(key_shared, (1, D), jnp.float32)
    noise = jax.random.normal(key_noise, (POOL, D), jnp.float32)
    base = 0.7 * shared + 0.7 * noise
    return jnp.clip(base / jnp.sqrt(jnp.float32(D)), -1.0, 1.0).astype(jnp.bfloat16)


def draw_class_ids(key, part):
    nblk = TOPK // K_LOC
    span = VOCAB // nblk
    stride = span // K_LOC
    key_order, key_pick, key_near, key_far = jax.random.split(key, 4)
    scores = jax.random.randint(key_order, (POOL, nblk, K_LOC), 0, 1 << 20) * K_LOC + jnp.arange(K_LOC, dtype=jnp.int32)
    slots = jnp.argsort(scores, axis=-1, stable=True).astype(jnp.int32)
    pick = jax.random.randint(key_pick, (POOL, nblk, K_LOC), 0, 4)
    near = jax.random.randint(key_near, (POOL, nblk, K_LOC), 0, 4)
    far = jax.random.randint(key_far, (POOL, nblk, K_LOC), 0, stride)
    offset = jnp.where(pick > 0, near, far)
    base = (jnp.arange(nblk, dtype=jnp.int32) * span).reshape(1, nblk, 1)
    ids = base + slots * stride + offset
    return ids.reshape(POOL, TOPK).astype(jnp.int32)


def levels(own_key, shape, cuts, smallest, high):
    level, own = 1.0, jax.random.fold_in(own_key, 6)
    for dim, shards_of in cuts:
        heights = jnp.exp(jax.random.uniform(jax.random.fold_in(own, dim), (shards_of,), jnp.float32, smallest / len(cuts), high / len(cuts)))
        level = level * jnp.repeat(heights, shape[dim] // shards_of).reshape([-1 if axis == dim else 1 for axis in range(len(shape))])
    return level


def setup_inputs(seed: int = 0) -> dict:
    key_list = jax.random.split(jax.random.key(seed), 5)
    hidden_states = draw_hidden_states(jax.random.fold_in(key_list[4], 71), 0)
    factor_values = jnp.clip(0.029907227 + 0.10974121 * jax.random.uniform(key_list[1], (POOL, TOPK), jnp.float32) ** levels(key_list[1], (POOL, TOPK), ((0, 16), (1, 8)), -0.2, 0.2), 0.029907227, 0.13964844).astype(jnp.bfloat16)
    class_ids = draw_class_ids(jax.random.fold_in(key_list[4], 71), 0)
    centers = jax.random.randint(key_list[3], (STEPS,), 0, POOL).astype(jnp.int32)
    return {"hidden_states": hidden_states, "factor_values": factor_values, "class_ids": class_ids, "centers": centers}


def reference(hidden_states, factor_values, class_ids, centers):
    nblk = TOPK // K_LOC
    vals = factor_values.astype(jnp.float32)
    sq_h = jnp.sum(jnp.square(hidden_states.astype(jnp.float32)), axis=1)
    sq_a = jnp.sum(vals * vals, axis=1)
    groups = POOL // SAMP_DEV
    means = []
    min_distance = None
    for step in range(STEPS):
        center = centers[step].astype(jnp.int32)
        h_row = lax.dynamic_slice_in_dim(hidden_states, center, 1, 0)[0]
        v_row = lax.dynamic_slice_in_dim(vals, center, 1, 0)[0]
        i_row = lax.dynamic_slice_in_dim(class_ids, center, 1, 0)[0]
        inner_h = jnp.dot(hidden_states, h_row, preferred_element_type=jnp.float32)

        def block(pair):
            values, idents = pair
            match = idents.reshape(-1, nblk, K_LOC, 1) == i_row.reshape(1, nblk, 1, K_LOC)
            prod = values.reshape(-1, nblk, K_LOC, 1) * v_row.reshape(1, nblk, 1, K_LOC)
            return jnp.sum(jnp.where(match, prod, jnp.float32(0.0)), axis=(1, 2, 3))

        inner_a = lax.map(block, (vals.reshape(groups, SAMP_DEV, TOPK), class_ids.reshape(groups, SAMP_DEV, TOPK))).reshape(POOL)
        norm_hc = jnp.sum(jnp.square(h_row.astype(jnp.float32)))
        norm_ac = jnp.sum(v_row * v_row)
        dist = jnp.maximum(sq_h * sq_a + norm_hc * norm_ac - 2.0 * inner_h * inner_a, jnp.float32(0.0))
        min_distance = dist if step == 0 else jnp.minimum(min_distance, dist)
        means.append(jnp.sum(min_distance) / POOL)
    return min_distance, jnp.stack(means)
```

```python
import functools

import jax
import jax.numpy as jnp
from jax import lax
from jax.experimental import pallas as pl
from jax.experimental.pallas import tpu as pltpu
from jax.sharding import PartitionSpec as P

STEPS = 3
VOCAB = 128256
MESH = pl.DeviceIdType.MESH
F32 = jnp.float32
BF16 = jnp.bfloat16
NT = (((1,), (1,)), ((), ()))


def iota(shape, dim):
    return lax.broadcasted_iota(jnp.int32, shape, dim)


def kernel(
    n_dp, n_mp, pool,
    h_hbm, v_hbm, i_hbm, cen, min_ref, mean_ref,
    h, v, ids, abuf, nbuf, bsend, bbuf, m1, m2,
    load_sem, a_send, a_recv, n_send, n_recv, b_send, b_recv, s1, r1, s2, r2,
):
    dp, mp = lax.axis_index("dp"), lax.axis_index("mp")
    groups, _, width = h.shape
    rows_all = groups * 16
    k_loc = v.shape[0]
    rows = rows_all // n_mp
    q_n = width // 128

    loads = [
        pltpu.make_async_copy(h_hbm, h, load_sem.at[0]),
        pltpu.make_async_copy(v_hbm, v, load_sem.at[1]),
        pltpu.make_async_copy(i_hbm, ids, load_sem.at[2]),
    ]
    for copy in loads:
        copy.start()

    barrier = pltpu.get_barrier_semaphore()
    for r in range(1, n_dp):
        pl.semaphore_signal(
            barrier, inc=1, device_id={"dp": lax.rem(dp + r, n_dp), "mp": mp}, device_id_type=MESH
        )
    for r in range(1, n_mp):
        pl.semaphore_signal(
            barrier, inc=1, device_id={"dp": dp, "mp": lax.rem(mp + r, n_mp)}, device_id_type=MESH
        )

    def send(src, dst, s_sem, r_sem, d, m):
        copy = pltpu.make_async_remote_copy(
            src_ref=src, dst_ref=dst, send_sem=s_sem, recv_sem=r_sem,
            device_id={"dp": d, "mp": m}, device_id_type=MESH,
        )
        copy.start()

    def settle(ref, s_sem, r_sem):
        return pltpu.make_async_remote_copy(
            src_ref=ref, dst_ref=ref, send_sem=s_sem, recv_sem=r_sem,
            device_id={"dp": dp, "mp": mp}, device_id_type=MESH,
        )

    for copy in loads:
        copy.wait()

    row16, lane16 = iota((16, 128), 0), iota((16, 128), 1)
    msg = jnp.zeros((16, 128), F32)
    wide = iota((16, rows_all), 1)
    base = mp * (VOCAB // n_mp)
    for j in range(STEPS):
        c = cen[j]
        loc = lax.rem(c, rows_all)
        mine = c - dp * rows_all
        start_r = loc - lax.rem(loc, 16)
        blk = h[lax.div(loc, 16)].astype(F32)
        pick_r = iota((16, width), 0) == mine - start_r
        row = jnp.sum(jnp.where(pick_r, blk, 0.0), axis=0, keepdims=True)
        for q in range(q_n):
            piece = row[:, q * 128 : (q + 1) * 128]
            msg = jnp.where(row16 == j * q_n + q, piece, msg)
        pick_l = wide == mine
        rel = jnp.sum(jnp.where(pick_l, ids[...] - base, 0), axis=1, keepdims=True)
        val = jnp.sum(jnp.where(pick_l, v[...].astype(F32), 0.0), axis=1, keepdims=True)
        hi = lax.shift_right_logical(rel, 7)
        lo = jnp.bitwise_and(rel, 127)
        parts = [val, hi.astype(F32), lo.astype(F32)]
        spread = jnp.zeros((16, 128), F32)
        for p, col in enumerate(parts):
            spread = jnp.where(lane16 == row16 + p * k_loc, col, spread)
        line = jnp.sum(spread, axis=0, keepdims=True)
        msg = jnp.where(row16 == STEPS * q_n + j, line, msg)
    abuf[dp] = msg.astype(BF16)

    pl.semaphore_wait(barrier, n_dp - 1 + n_mp - 1)
    for r in range(1, n_dp):
        send(abuf.at[dp], abuf.at[dp], a_send, a_recv, lax.rem(dp + r, n_dp), mp)

    ones = jnp.ones((16, 256), BF16)
    for r in range(n_mp):
        hc = h[pl.ds(r * (rows // 16), rows // 16)].reshape(rows, width).astype(F32)
        sq = hc * hc
        part = sq[:, 0:128]
        for q in range(1, q_n):
            part = part + sq[:, q * 128 : (q + 1) * 128]
        hi = part.astype(BF16)
        lo = (part - hi.astype(F32)).astype(BF16)
        both = jnp.concatenate([hi, lo], axis=1)
        sums = lax.dot_general(ones, both, NT, preferred_element_type=F32)
        bsend[r, 0:1, :] = sums[0:1, :]
        vc = v[:, pl.ds(r * rows, rows)].astype(F32)
        bsend[r, 1:2, :] = jnp.sum(vc * vc, axis=0, keepdims=True)

    settle(abuf.at[pl.ds(0, n_dp - 1)], a_send, a_recv).wait_recv()
    tot = jnp.zeros((16, 128), F32)
    for d in range(n_dp):
        tot = tot + abuf[d].astype(F32)

    keep = jnp.logical_or(row16 < STEPS * q_n, lane16 < k_loc)
    sums = jnp.sum(jnp.where(keep, tot * tot, 0.0), axis=1, keepdims=True)
    first = jnp.logical_and(row16 < STEPS * q_n, lane16 == lax.shift_right_logical(row16, 2))
    second = jnp.logical_and(row16 >= STEPS * q_n, lane16 == row16 - STEPS * q_n + 8)
    line = jnp.sum(jnp.where(jnp.logical_or(first, second), sums, 0.0), axis=0, keepdims=True)
    nbuf[mp] = line
    for r in range(1, n_mp):
        send(nbuf.at[mp], nbuf.at[mp], n_send, n_recv, dp, lax.rem(mp + r, n_mp))

    row8 = iota((16, 128), 0)
    cparts = []
    for q in range(q_n):
        part = jnp.zeros((16, 128), F32)
        for j in range(STEPS):
            part = jnp.where(row8 == j, tot[j * q_n + q : j * q_n + q + 1, :], part)
        cparts.append(part)
    cmat = jnp.concatenate(cparts, axis=1).astype(BF16)

    cvals, cids = [], []
    for j in range(STEPS):
        line = tot[STEPS * q_n + j : STEPS * q_n + j + 1, :]
        for k in range(k_loc):
            cvals.append(line[:, k : k + 1])
            hi = line[:, k_loc + k : k_loc + k + 1]
            lo = line[:, 2 * k_loc + k : 2 * k_loc + k + 1]
            cids.append((hi * 128.0 + lo).astype(jnp.int32) + base)

    for r in list(range(1, n_mp)) + [0]:
        to = lax.rem(mp + r, n_mp)
        start = pl.multiple_of(to * rows, rows)
        hc = h[pl.ds(to * (rows // 16), rows // 16)].reshape(rows, width)
        inner = lax.dot_general(cmat, hc, NT, preferred_element_type=F32)
        bsend[to, 2 : 2 + STEPS, :] = inner[0:STEPS, :]
        vc = v[:, pl.ds(start, rows)].astype(F32)
        ic = ids[:, pl.ds(start, rows)]
        for j in range(STEPS):
            w = jnp.zeros((k_loc, rows), F32)
            for k in range(k_loc):
                w = jnp.where(ic == cids[j * k_loc + k], cvals[j * k_loc + k], w)
            bsend[to, 2 + STEPS + j : 3 + STEPS + j, :] = jnp.sum(vc * w, axis=0, keepdims=True)
        if r:
            send(bsend.at[to], bbuf.at[mp], b_send, b_recv, dp, to)
    bbuf[mp] = bsend[mp]

    settle(nbuf.at[pl.ds(0, n_mp - 1)], n_send, n_recv).wait_recv()
    settle(bbuf.at[pl.ds(0, n_mp - 1)], b_send, b_recv).wait_recv()
    full, norms = bbuf[0], nbuf[0]
    for m in range(1, n_mp):
        full = full + bbuf[m]
        norms = norms + nbuf[m]

    both = full[0:1, :] * full[1:2, :]
    lane = iota((1, 128), 1)
    line = jnp.zeros((1, 128), F32)
    least = None
    for j in range(STEPS):
        own = norms[:, j : j + 1] * norms[:, 8 + j : 9 + j]
        cross = 2.0 * full[2 + j : 3 + j, :] * full[2 + STEPS + j : 3 + STEPS + j, :]
        dist = jnp.maximum(both + own - cross, 0.0)
        least = dist if j == 0 else jnp.minimum(least, dist)
        line = jnp.where(lane == j, jnp.sum(least, axis=1, keepdims=True), line)
    min_ref[...] = least

    m1[mp] = line
    for r in range(1, n_mp):
        send(m1.at[mp], m1.at[mp], s1, r1, dp, lax.rem(mp + r, n_mp))
    settle(m1.at[pl.ds(0, n_mp - 1)], s1, r1).wait_recv()
    line = m1[0]
    for m in range(1, n_mp):
        line = line + m1[m]
    m2[dp] = line
    for r in range(1, n_dp):
        send(m2.at[dp], m2.at[dp], s2, r2, lax.rem(dp + r, n_dp), mp)
    settle(m2.at[pl.ds(0, n_dp - 1)], s2, r2).wait_recv()
    line = m2[0]
    for d in range(1, n_dp):
        line = line + m2[d]
    mean_ref[...] = line * (1.0 / pool)

    settle(abuf.at[pl.ds(0, n_dp - 1)], a_send, a_recv).wait_send()
    settle(nbuf.at[pl.ds(0, n_mp - 1)], n_send, n_recv).wait_send()
    settle(bbuf.at[pl.ds(0, n_mp - 1)], b_send, b_recv).wait_send()
    settle(m1.at[pl.ds(0, n_mp - 1)], s1, r1).wait_send()
    settle(m2.at[pl.ds(0, n_dp - 1)], s2, r2).wait_send()


def body(n_dp, n_mp, hidden_states, factor_values, class_ids, centers):
    rows_all, width = hidden_states.shape
    k_loc = factor_values.shape[1]
    rows = rows_all // n_mp
    dma = pltpu.SemaphoreType.DMA
    least, means = pl.pallas_call(
        functools.partial(kernel, n_dp, n_mp, rows_all * n_dp),
        out_shape=(
            jax.ShapeDtypeStruct((1, rows), F32),
            jax.ShapeDtypeStruct((1, 128), F32),
        ),
        in_specs=[pl.BlockSpec(memory_space=pl.ANY)] * 3
        + [pl.BlockSpec(memory_space=pltpu.SMEM)],
        out_specs=(pl.BlockSpec(memory_space=pltpu.VMEM),) * 2,
        scratch_shapes=[
            pltpu.VMEM((rows_all // 16, 16, width), BF16),
            pltpu.VMEM((k_loc, rows_all), BF16),
            pltpu.VMEM((k_loc, rows_all), jnp.int32),
            pltpu.VMEM((n_dp, 16, 128), BF16),
            pltpu.VMEM((n_mp, 1, 128), F32),
            pltpu.VMEM((n_mp, 8, rows), F32),
            pltpu.VMEM((n_mp, 8, rows), F32),
            pltpu.VMEM((n_mp, 1, 128), F32),
            pltpu.VMEM((n_dp, 1, 128), F32),
            dma((3,)),
        ]
        + [dma(())] * 10,
        compiler_params=pltpu.CompilerParams(collective_id=0, has_side_effects=True),
        name="badge",
    )(hidden_states.reshape(rows_all // 16, 16, width), factor_values.T, class_ids.T, centers)
    return least.reshape(rows), means[0, :STEPS]


def solution(mesh):
    return jax.shard_map(
        functools.partial(body, mesh.shape["dp"], mesh.shape["mp"]),
        mesh=mesh,
        in_specs=(P("dp", "mp"), P("dp", "mp"), P("dp", "mp"), P()),
        out_specs=(P(("dp", "mp")), P()),
        check_vma=False,
    )
```

```python
import functools
import itertools

import jax
import jax.numpy as jnp
from jax import lax
from jax.experimental import pallas as pl
from jax.experimental.pallas import tpu as pltpu
from jax.sharding import PartitionSpec as P

STEPS = 3
VOCAB = 128256
MESH = pl.DeviceIdType.MESH
F32 = jnp.float32
BF16 = jnp.bfloat16
NT = (((1,), (1,)), ((), ()))


def iota(shape, dim):
    return lax.broadcasted_iota(jnp.int32, shape, dim)


def kernel(
    n_dp, n_mp, pool,
    h_hbm, v_hbm, i_hbm, c_hbm, min_ref, mean_ref,
    h, v, ids, cen, abuf, nbuf, bsend, bbuf, mbuf,
    load_sem, a_send, a_recv, n_send, n_recv, b_send, b_recv, m_send, m_recv,
):
    dp, mp = lax.axis_index("dp"), lax.axis_index("mp")
    groups, _, width = h.shape
    rows_all = groups * 16
    k_loc = v.shape[0]
    rows = rows_all // n_mp
    q_n = width // 128

    loads = [
        pltpu.make_async_copy(h_hbm, h, load_sem.at[0]),
        pltpu.make_async_copy(v_hbm, v, load_sem.at[1]),
        pltpu.make_async_copy(i_hbm, ids, load_sem.at[2]),
        pltpu.make_async_copy(c_hbm, cen, load_sem.at[3]),
    ]
    for copy in loads:
        copy.start()

    core, x, y_hi = lax.rem(dp, 2), lax.rem(lax.div(dp, 2), 4), lax.div(dp, 8)
    y_lo, z = lax.rem(mp, 2), lax.div(mp, 2)
    dp_at = [
        (lax.rem(y_hi + a, 2) * 4 + lax.rem(x + b, 4)) * 2 + lax.rem(core + c, 2)
        for a, b, c in sorted(
            itertools.product(range(2), range(4), range(2)),
            key=lambda t: -(4 * t[0] + 2 * min(t[1], 4 - t[1]) + t[2]),
        )[:-1]
    ]
    mp_at = [
        lax.rem(z + a, 4) * 2 + lax.rem(y_lo + b, 2)
        for a, b in sorted(
            itertools.product(range(4), range(2)), key=lambda t: -(min(t[0], 4 - t[0]) + t[1])
        )[:-1]
    ]
    barrier = pltpu.get_barrier_semaphore()
    for d in dp_at:
        pl.semaphore_signal(barrier, inc=1, device_id={"dp": d, "mp": mp}, device_id_type=MESH)
    for m in mp_at:
        pl.semaphore_signal(barrier, inc=1, device_id={"dp": dp, "mp": m}, device_id_type=MESH)

    def send(src, dst, s_sem, r_sem, d, m):
        copy = pltpu.make_async_remote_copy(
            src_ref=src, dst_ref=dst, send_sem=s_sem, recv_sem=r_sem,
            device_id={"dp": d, "mp": m}, device_id_type=MESH,
        )
        copy.start()

    def settle(ref, s_sem, r_sem):
        return pltpu.make_async_remote_copy(
            src_ref=ref, dst_ref=ref, send_sem=s_sem, recv_sem=r_sem,
            device_id={"dp": dp, "mp": mp}, device_id_type=MESH,
        )

    for copy in loads:
        copy.wait()

    row16, lane16 = iota((16, 128), 0), iota((16, 128), 1)
    msg = jnp.zeros((16, 128), F32)
    wide = iota((16, rows_all), 1)
    base = mp * (VOCAB // n_mp)
    for j in range(STEPS):
        c = cen[j]
        loc = lax.rem(c, rows_all)
        mine = c - dp * rows_all
        start_r = loc - lax.rem(loc, 16)
        blk = h[lax.div(loc, 16)].astype(F32)
        pick_r = iota((16, width), 0) == mine - start_r
        row = jnp.sum(jnp.where(pick_r, blk, 0.0), axis=0, keepdims=True)
        for q in range(q_n):
            piece = row[:, q * 128 : (q + 1) * 128]
            msg = jnp.where(row16 == j * q_n + q, piece, msg)
        pick_l = wide == mine
        rel = jnp.sum(jnp.where(pick_l, ids[...] - base, 0), axis=1, keepdims=True)
        val = jnp.sum(jnp.where(pick_l, v[...].astype(F32), 0.0), axis=1, keepdims=True)
        hi = lax.shift_right_logical(rel, 7)
        lo = jnp.bitwise_and(rel, 127)
        parts = [val, hi.astype(F32), lo.astype(F32)]
        spread = jnp.zeros((16, 128), F32)
        for p, col in enumerate(parts):
            spread = jnp.where(lane16 == row16 + p * k_loc, col, spread)
        line = jnp.sum(spread, axis=0, keepdims=True)
        msg = jnp.where(row16 == STEPS * q_n + j, line, msg)
    abuf[dp] = msg.astype(BF16)

    pl.semaphore_wait(barrier, n_dp - 1 + n_mp - 1)
    for d in dp_at:
        send(abuf.at[dp], abuf.at[dp], a_send, a_recv, d, mp)

    ones = jnp.ones((16, 256), BF16)
    for r in range(n_mp):
        hc = h[pl.ds(r * (rows // 16), rows // 16)].reshape(rows, width).astype(F32)
        sq = hc * hc
        part = sq[:, 0:128]
        for q in range(1, q_n):
            part = part + sq[:, q * 128 : (q + 1) * 128]
        hi = part.astype(BF16)
        lo = (part - hi.astype(F32)).astype(BF16)
        both = jnp.concatenate([hi, lo], axis=1)
        sums = lax.dot_general(ones, both, NT, preferred_element_type=F32)
        bsend[r, 0:1, :] = sums[0:1, :]
        vc = v[:, pl.ds(r * rows, rows)].astype(F32)
        bsend[r, 1:2, :] = jnp.sum(vc * vc, axis=0, keepdims=True)

    settle(abuf.at[pl.ds(0, n_dp - 1)], a_send, a_recv).wait_recv()
    tot = jnp.zeros((16, 128), F32)
    for d in range(n_dp):
        tot = tot + abuf[d].astype(F32)

    keep = jnp.logical_or(row16 < STEPS * q_n, lane16 < k_loc)
    sums = jnp.sum(jnp.where(keep, tot * tot, 0.0), axis=1, keepdims=True)
    first = jnp.logical_and(row16 < STEPS * q_n, lane16 == lax.shift_right_logical(row16, 2))
    second = jnp.logical_and(row16 >= STEPS * q_n, lane16 == row16 - STEPS * q_n + 8)
    line = jnp.sum(jnp.where(jnp.logical_or(first, second), sums, 0.0), axis=0, keepdims=True)
    nbuf[mp] = line
    for m in mp_at:
        send(nbuf.at[mp], nbuf.at[mp], n_send, n_recv, dp, m)

    row8 = iota((16, 128), 0)
    cparts = []
    for q in range(q_n):
        part = jnp.zeros((16, 128), F32)
        for j in range(STEPS):
            part = jnp.where(row8 == j, tot[j * q_n + q : j * q_n + q + 1, :], part)
        cparts.append(part)
    cmat = jnp.concatenate(cparts, axis=1).astype(BF16)

    cvals, cids = [], []
    for j in range(STEPS):
        line = tot[STEPS * q_n + j : STEPS * q_n + j + 1, :]
        for k in range(k_loc):
            cvals.append(line[:, k : k + 1])
            hi = line[:, k_loc + k : k_loc + k + 1]
            lo = line[:, 2 * k_loc + k : 2 * k_loc + k + 1]
            cids.append((hi * 128.0 + lo).astype(jnp.int32) + base)

    def inner(to):
        hc = h[pl.ds(to * (rows // 16), rows // 16)].reshape(rows, width)
        return lax.dot_general(cmat, hc, NT, preferred_element_type=F32)

    order = mp_at + [mp]
    ahead = inner(order[0])
    for n, to in enumerate(order):
        now = ahead
        if n + 1 < n_mp:
            ahead = inner(order[n + 1])
        start = pl.multiple_of(to * rows, rows)
        vc = v[:, pl.ds(start, rows)].astype(F32)
        ic = ids[:, pl.ds(start, rows)]
        found = []
        for j in range(STEPS):
            w = jnp.zeros((k_loc, rows), F32)
            for k in range(k_loc):
                w = jnp.where(ic == cids[j * k_loc + k], cvals[j * k_loc + k], w)
            found.append(jnp.sum(vc * w, axis=0, keepdims=True))
        bsend[to, 2 : 2 + STEPS, :] = now[0:STEPS, :]
        for j in range(STEPS):
            bsend[to, 2 + STEPS + j : 3 + STEPS + j, :] = found[j]
        if n + 1 < n_mp:
            send(bsend.at[to], bbuf.at[mp], b_send, b_recv, dp, to)
    bbuf[mp] = bsend[mp]

    settle(nbuf.at[pl.ds(0, n_mp - 1)], n_send, n_recv).wait_recv()
    settle(bbuf.at[pl.ds(0, n_mp - 1)], b_send, b_recv).wait_recv()
    full, norms = bbuf[0], nbuf[0]
    for m in range(1, n_mp):
        full = full + bbuf[m]
        norms = norms + nbuf[m]

    both = full[0:1, :] * full[1:2, :]
    lane = iota((1, 128), 1)
    line = jnp.zeros((1, 128), F32)
    least = None
    for j in range(STEPS):
        own = norms[:, j : j + 1] * norms[:, 8 + j : 9 + j]
        cross = 2.0 * full[2 + j : 3 + j, :] * full[2 + STEPS + j : 3 + STEPS + j, :]
        dist = jnp.maximum(both + own - cross, 0.0)
        least = dist if j == 0 else jnp.minimum(least, dist)
        line = jnp.where(lane == j, jnp.sum(least, axis=1, keepdims=True), line)
    min_ref[...] = least

    me = dp * n_mp + mp
    mbuf[me] = line
    moves = sorted(
        itertools.product(range(4), range(4), range(4), range(2)),
        key=lambda t: -(2 * sum(min(u, 4 - u) for u in t[:3]) + t[3]),
    )[:-1]
    xs = [lax.rem(x + a, 4) * (2 * n_mp) for a in range(4)]
    ys = [lax.rem(y_hi * 2 + y_lo + a, 4) for a in range(4)]
    ys = [lax.div(y, 2) * (8 * n_mp) + lax.rem(y, 2) for y in ys]
    zs = [lax.rem(z + a, 4) * 2 for a in range(4)]
    cs = [lax.rem(core + a, 2) * n_mp for a in range(2)]
    for a, b, c, e in moves:
        copy = pltpu.make_async_remote_copy(
            src_ref=mbuf.at[me], dst_ref=mbuf.at[me], send_sem=m_send, recv_sem=m_recv,
            device_id=xs[a] + ys[b] + zs[c] + cs[e], device_id_type=pl.DeviceIdType.LOGICAL,
        )
        copy.start()
    settle(mbuf.at[pl.ds(0, n_dp * n_mp - 1)], m_send, m_recv).wait_recv()
    line = mbuf[0]
    for d in range(1, n_dp * n_mp):
        line = line + mbuf[d]
    mean_ref[...] = line * (1.0 / pool)

    settle(abuf.at[pl.ds(0, n_dp - 1)], a_send, a_recv).wait_send()
    settle(nbuf.at[pl.ds(0, n_mp - 1)], n_send, n_recv).wait_send()
    settle(bbuf.at[pl.ds(0, n_mp - 1)], b_send, b_recv).wait_send()
    settle(mbuf.at[pl.ds(0, n_dp * n_mp - 1)], m_send, m_recv).wait_send()


def body(n_dp, n_mp, hidden_states, factor_values, class_ids, centers):
    rows_all, width = hidden_states.shape
    k_loc = factor_values.shape[1]
    rows = rows_all // n_mp
    dma = pltpu.SemaphoreType.DMA
    least, means = pl.pallas_call(
        functools.partial(kernel, n_dp, n_mp, rows_all * n_dp),
        out_shape=(
            pltpu.VMEM((1, rows), F32),
            pltpu.VMEM((1, 128), F32),
        ),
        in_specs=[pl.BlockSpec(memory_space=pl.ANY)] * 4,
        out_specs=(pl.BlockSpec(memory_space=pltpu.VMEM),) * 2,
        scratch_shapes=[
            pltpu.VMEM((rows_all // 16, 16, width), BF16),
            pltpu.VMEM((k_loc, rows_all), BF16),
            pltpu.VMEM((k_loc, rows_all), jnp.int32),
            pltpu.SMEM((STEPS,), jnp.int32),
            pltpu.VMEM((n_dp, 16, 128), BF16),
            pltpu.VMEM((n_mp, 1, 128), F32),
            pltpu.VMEM((n_mp, 8, rows), F32),
            pltpu.VMEM((n_mp, 8, rows), F32),
            pltpu.VMEM((n_dp * n_mp, 1, 128), F32),
            dma((4,)),
        ]
        + [dma(())] * 8,
        compiler_params=pltpu.CompilerParams(collective_id=0, has_side_effects=True),
        name="badge",
    )(hidden_states.reshape(rows_all // 16, 16, width), factor_values.T, class_ids.T, centers)
    return least.reshape(rows), means[0, :STEPS]


def solution(mesh):
    return jax.shard_map(
        functools.partial(body, mesh.shape["dp"], mesh.shape["mp"]),
        mesh=mesh,
        in_specs=(P("dp", "mp"), P("dp", "mp"), P("dp", "mp"), P()),
        out_specs=(P(("dp", "mp")), P()),
        check_vma=False,
    )
```

```python
import functools
import itertools

import jax
import jax.numpy as jnp
from jax import lax
from jax.experimental import pallas as pl
from jax.experimental.pallas import tpu as pltpu
from jax.sharding import PartitionSpec as P

STEPS = 3
VOCAB = 128256
MESH = pl.DeviceIdType.MESH
F32 = jnp.float32
BF16 = jnp.bfloat16
NT = (((1,), (1,)), ((), ()))


def iota(shape, dim):
    return lax.broadcasted_iota(jnp.int32, shape, dim)


def kernel(
    n_dp, n_mp, pool,
    h_hbm, v_hbm, i_hbm, c_hbm, min_ref, mean_ref,
    h, v, ids, cen, abuf, nbuf, bsend, bbuf, mbuf,
    load_sem, a_send, a_recv, n_send, n_recv, b_send, b_recv, m_send, m_recv,
):
    dp, mp = lax.axis_index("dp"), lax.axis_index("mp")
    groups, _, width = h.shape
    rows_all = groups * 16
    k_loc = v.shape[0]
    rows = rows_all // n_mp
    q_n = width // 128

    loads = [
        pltpu.make_async_copy(h_hbm, h, load_sem.at[0]),
        pltpu.make_async_copy(v_hbm, v, load_sem.at[1]),
        pltpu.make_async_copy(i_hbm, ids, load_sem.at[2]),
        pltpu.make_async_copy(c_hbm, cen, load_sem.at[3]),
    ]
    for copy in loads:
        copy.start()

    core, x, y_hi = lax.rem(dp, 2), lax.rem(lax.div(dp, 2), 4), lax.div(dp, 8)
    y_lo, z = lax.rem(mp, 2), lax.div(mp, 2)
    dp_at = [
        (lax.rem(y_hi + a, 2) * 4 + lax.rem(x + b, 4)) * 2 + lax.rem(core + c, 2)
        for a, b, c in sorted(
            itertools.product(range(2), range(4), range(2)),
            key=lambda t: -(4 * t[0] + 2 * min(t[1], 4 - t[1]) + t[2]),
        )[:-1]
    ]
    mp_at = [
        lax.rem(z + a, 4) * 2 + lax.rem(y_lo + b, 2)
        for a, b in sorted(
            itertools.product(range(4), range(2)), key=lambda t: -(min(t[0], 4 - t[0]) + t[1])
        )[:-1]
    ]
    barrier = pltpu.get_barrier_semaphore()
    for d in dp_at:
        pl.semaphore_signal(barrier, inc=1, device_id={"dp": d, "mp": mp}, device_id_type=MESH)
    for m in mp_at:
        pl.semaphore_signal(barrier, inc=1, device_id={"dp": dp, "mp": m}, device_id_type=MESH)

    def send(src, dst, s_sem, r_sem, d, m):
        copy = pltpu.make_async_remote_copy(
            src_ref=src, dst_ref=dst, send_sem=s_sem, recv_sem=r_sem,
            device_id={"dp": d, "mp": m}, device_id_type=MESH,
        )
        copy.start()

    def settle(ref, s_sem, r_sem):
        return pltpu.make_async_remote_copy(
            src_ref=ref, dst_ref=ref, send_sem=s_sem, recv_sem=r_sem,
            device_id={"dp": dp, "mp": mp}, device_id_type=MESH,
        )

    for copy in loads:
        copy.wait()

    row16, lane16 = iota((16, 128), 0), iota((16, 128), 1)
    msg = jnp.zeros((16, 128), F32)
    wide = iota((16, rows_all), 1)
    base = mp * (VOCAB // n_mp)
    for j in range(STEPS):
        c = cen[j]
        loc = lax.rem(c, rows_all)
        mine = c - dp * rows_all
        start_r = loc - lax.rem(loc, 16)
        blk = h[lax.div(loc, 16)].astype(F32)
        pick_r = iota((16, width), 0) == mine - start_r
        row = jnp.sum(jnp.where(pick_r, blk, 0.0), axis=0, keepdims=True)
        for q in range(q_n):
            piece = row[:, q * 128 : (q + 1) * 128]
            msg = jnp.where(row16 == j * q_n + q, piece, msg)
        pick_l = wide == mine
        rel = jnp.sum(jnp.where(pick_l, ids[...] - base, 0), axis=1, keepdims=True)
        val = jnp.sum(jnp.where(pick_l, v[...].astype(F32), 0.0), axis=1, keepdims=True)
        hi = lax.shift_right_logical(rel, 7)
        lo = jnp.bitwise_and(rel, 127)
        parts = [val, hi.astype(F32), lo.astype(F32)]
        spread = jnp.zeros((16, 128), F32)
        for p, col in enumerate(parts):
            spread = jnp.where(lane16 == row16 + p * k_loc, col, spread)
        line = jnp.sum(spread, axis=0, keepdims=True)
        msg = jnp.where(row16 == STEPS * q_n + j, line, msg)
    abuf[dp] = msg.astype(BF16)

    pl.semaphore_wait(barrier, n_dp - 1 + n_mp - 1)
    for d in dp_at:
        send(abuf.at[dp], abuf.at[dp], a_send, a_recv, d, mp)

    ones = jnp.ones((16, 256), BF16)
    for r in range(n_mp):
        hc = h[pl.ds(r * (rows // 16), rows // 16)].reshape(rows, width).astype(F32)
        sq = hc * hc
        part = sq[:, 0:128]
        for q in range(1, q_n):
            part = part + sq[:, q * 128 : (q + 1) * 128]
        hi = part.astype(BF16)
        lo = (part - hi.astype(F32)).astype(BF16)
        both = jnp.concatenate([hi, lo], axis=1)
        sums = lax.dot_general(ones, both, NT, preferred_element_type=F32)
        bsend[r, 0:1, :] = sums[0:1, :]
        vc = v[:, pl.ds(r * rows, rows)].astype(F32)
        bsend[r, 1:2, :] = jnp.sum(vc * vc, axis=0, keepdims=True)

    settle(abuf.at[pl.ds(0, n_dp - 1)], a_send, a_recv).wait_recv()
    tot = jnp.zeros((16, 128), F32)
    for d in range(n_dp):
        tot = tot + abuf[d].astype(F32)

    keep = jnp.logical_or(row16 < STEPS * q_n, lane16 < k_loc)
    sums = jnp.sum(jnp.where(keep, tot * tot, 0.0), axis=1, keepdims=True)
    first = jnp.logical_and(row16 < STEPS * q_n, lane16 == lax.shift_right_logical(row16, 2))
    second = jnp.logical_and(row16 >= STEPS * q_n, lane16 == row16 - STEPS * q_n + 8)
    line = jnp.sum(jnp.where(jnp.logical_or(first, second), sums, 0.0), axis=0, keepdims=True)
    nbuf[mp] = line
    for m in mp_at:
        send(nbuf.at[mp], nbuf.at[mp], n_send, n_recv, dp, m)

    row8 = iota((16, 128), 0)
    cparts = []
    for q in range(q_n):
        part = jnp.zeros((16, 128), F32)
        for j in range(STEPS):
            part = jnp.where(row8 == j, tot[j * q_n + q : j * q_n + q + 1, :], part)
        cparts.append(part)
    cmat = jnp.concatenate(cparts, axis=1).astype(BF16)

    cvals, cids = [], []
    for j in range(STEPS):
        line = tot[STEPS * q_n + j : STEPS * q_n + j + 1, :]
        for k in range(k_loc):
            cvals.append(line[:, k : k + 1])
            hi = line[:, k_loc + k : k_loc + k + 1]
            lo = line[:, 2 * k_loc + k : 2 * k_loc + k + 1]
            cids.append((hi * 128.0 + lo).astype(jnp.int32) + base)

    def inner(to):
        hc = h[pl.ds(to * (rows // 16), rows // 16)].reshape(rows, width)
        return lax.dot_general(cmat, hc, NT, preferred_element_type=F32)

    order = mp_at + [mp]
    ahead = inner(order[0])
    for n, to in enumerate(order):
        now = ahead
        if n + 1 < n_mp:
            ahead = inner(order[n + 1])
        start = pl.multiple_of(to * rows, rows)
        vc = v[:, pl.ds(start, rows)].astype(F32)
        ic = ids[:, pl.ds(start, rows)]
        found = []
        for j in range(STEPS):
            w = jnp.zeros((k_loc, rows), F32)
            for k in range(k_loc):
                w = jnp.where(ic == cids[j * k_loc + k], cvals[j * k_loc + k], w)
            found.append(jnp.sum(vc * w, axis=0, keepdims=True))
        bsend[to, 2 : 2 + STEPS, :] = now[0:STEPS, :]
        for j in range(STEPS):
            bsend[to, 2 + STEPS + j : 3 + STEPS + j, :] = found[j]
        if n + 1 < n_mp:
            send(bsend.at[to], bbuf.at[mp], b_send, b_recv, dp, to)
    bbuf[mp] = bsend[mp]

    settle(nbuf.at[pl.ds(0, n_mp - 1)], n_send, n_recv).wait_recv()
    settle(bbuf.at[pl.ds(0, n_mp - 1)], b_send, b_recv).wait_recv()
    full, norms = bbuf[0], nbuf[0]
    for m in range(1, n_mp):
        full = full + bbuf[m]
        norms = norms + nbuf[m]

    both = full[0:1, :] * full[1:2, :]
    lane = iota((1, 128), 1)
    line = jnp.zeros((1, 128), F32)
    least = None
    for j in range(STEPS):
        own = norms[:, j : j + 1] * norms[:, 8 + j : 9 + j]
        cross = 2.0 * full[2 + j : 3 + j, :] * full[2 + STEPS + j : 3 + STEPS + j, :]
        dist = jnp.maximum(both + own - cross, 0.0)
        least = dist if j == 0 else jnp.minimum(least, dist)
        line = jnp.where(lane == j, jnp.sum(least, axis=1, keepdims=True), line)
    min_ref[...] = least

    me = dp * n_mp + mp
    mbuf[me] = line
    moves = sorted(
        itertools.product(range(4), range(4), range(4), range(2)),
        key=lambda t: -(2 * sum(min(u, 4 - u) for u in t[:3]) + t[3]),
    )[:-1]
    xs = [lax.rem(x + a, 4) * (2 * n_mp) for a in range(4)]
    ys = [lax.rem(y_hi * 2 + y_lo + a, 4) for a in range(4)]
    ys = [lax.div(y, 2) * (8 * n_mp) + lax.rem(y, 2) for y in ys]
    zs = [lax.rem(z + a, 4) * 2 for a in range(4)]
    cs = [lax.rem(core + a, 2) * n_mp for a in range(2)]
    for a, b, c, e in moves:
        copy = pltpu.make_async_remote_copy(
            src_ref=mbuf.at[me], dst_ref=mbuf.at[me], send_sem=m_send, recv_sem=m_recv,
            device_id=xs[a] + ys[b] + zs[c] + cs[e], device_id_type=pl.DeviceIdType.LOGICAL,
        )
        copy.start()
    settle(mbuf.at[pl.ds(0, n_dp * n_mp - 1)], m_send, m_recv).wait_recv()
    line = mbuf[0]
    for d in range(1, n_dp * n_mp):
        line = line + mbuf[d]
    mean_ref[...] = line[:, 0:STEPS] * (1.0 / pool)

    settle(abuf.at[pl.ds(0, n_dp - 1)], a_send, a_recv).wait_send()
    settle(nbuf.at[pl.ds(0, n_mp - 1)], n_send, n_recv).wait_send()
    settle(bbuf.at[pl.ds(0, n_mp - 1)], b_send, b_recv).wait_send()
    settle(mbuf.at[pl.ds(0, n_dp * n_mp - 1)], m_send, m_recv).wait_send()


def put(least_ref, mean_ref, least_hbm, mean_hbm, sem):
    copies = [
        pltpu.make_async_copy(least_ref, least_hbm, sem.at[0]),
        pltpu.make_async_copy(mean_ref, mean_hbm, sem.at[1]),
    ]
    for copy in copies:
        copy.start()
    for copy in copies:
        copy.wait()


def body(n_dp, n_mp, hidden_states, factor_values, class_ids, centers):
    rows_all, width = hidden_states.shape
    k_loc = factor_values.shape[1]
    rows = rows_all // n_mp
    dma = pltpu.SemaphoreType.DMA
    least, means = pl.pallas_call(
        functools.partial(kernel, n_dp, n_mp, rows_all * n_dp),
        out_shape=(
            pltpu.VMEM((1, rows), F32),
            pltpu.VMEM((1, STEPS), F32),
        ),
        in_specs=[pl.BlockSpec(memory_space=pl.ANY)] * 4,
        out_specs=(pl.BlockSpec(memory_space=pltpu.VMEM),) * 2,
        scratch_shapes=[
            pltpu.VMEM((rows_all // 16, 16, width), BF16),
            pltpu.VMEM((k_loc, rows_all), BF16),
            pltpu.VMEM((k_loc, rows_all), jnp.int32),
            pltpu.SMEM((STEPS,), jnp.int32),
            pltpu.VMEM((n_dp, 16, 128), BF16),
            pltpu.VMEM((n_mp, 1, 128), F32),
            pltpu.VMEM((n_mp, 8, rows), F32),
            pltpu.VMEM((n_mp, 8, rows), F32),
            pltpu.VMEM((n_dp * n_mp, 1, 128), F32),
            dma((4,)),
        ]
        + [dma(())] * 8,
        compiler_params=pltpu.CompilerParams(collective_id=0, has_side_effects=True),
        name="badge",
    )(hidden_states.reshape(rows_all // 16, 16, width), factor_values.T, class_ids.T, centers)
    least, means = pl.pallas_call(
        put,
        out_shape=(
            jax.ShapeDtypeStruct((1, rows), F32),
            jax.ShapeDtypeStruct((1, STEPS), F32),
        ),
        in_specs=[pl.BlockSpec(memory_space=pltpu.VMEM)] * 2,
        out_specs=(pl.BlockSpec(memory_space=pl.ANY),) * 2,
        scratch_shapes=[dma((2,))],
        name="put",
    )(*(pltpu.with_memory_space_constraint(a, pltpu.VMEM) for a in (least, means)))
    return least.reshape(rows), means.reshape(STEPS)


def solution(mesh):
    return jax.shard_map(
        functools.partial(body, mesh.shape["dp"], mesh.shape["mp"]),
        mesh=mesh,
        in_specs=(P("dp", "mp"), P("dp", "mp"), P("dp", "mp"), P()),
        out_specs=(P(("dp", "mp")), P()),
        check_vma=False,
    )
```
